128 devices in a mesh: dp: 1, tp: 2 (over core), cp: 64 (over z, y, x).
Axes of the slice: x: 4, y: 4, z: 4, core: 2. Of those that a mesh axis runs over, the one named last changes fastest.
Arguments:
- x: bfloat16 [4096, 2048], P(('dp', 'cp', 'tp'))
- pos: int32 [4096], P(('dp', 'cp', 'tp'))
- g1: bfloat16 [2048], replicated
- g2: bfloat16 [2048], replicated
- wq: bfloat16 [2048, 2048], P(None, 'tp')
- wk: bfloat16 [2048, 256], P(None, 'tp')
- wv: bfloat16 [2048, 256], P(None, 'tp')
- wo: bfloat16 [2048, 2048], P('tp')
- w1: bfloat16 [2048, 11008], P(None, 'tp')
- w3: bfloat16 [2048, 11008], P(None, 'tp')
- w2: bfloat16 [11008, 2048], P('tp')
Outputs:
- output: bfloat16 [4096, 2048], P(('dp', 'cp', 'tp'))
All inputs are finite; a program needn't handle non-finite values.
Results may differ from the reference program's by a relative error of at most 0.0111242.
Values are sent between devices in bfloat16 or wider.
A program may use at most 1 GiB of HBM per device.

```python
import math
import jax
import jax.numpy as jnp
from jax import lax

T = 4096
D = 2048
HQ = 16
HKV = 2
DH = 128
F = 11008
NDEV = 128
QB = 64
PIECE = T // (2 * NDEV)
GRP = HQ // HKV
EPS = 1e-5
THETA = 500000.0


def setup_inputs(seed: int = 0, part: int = 0) -> dict:
    kpart = jax.random.fold_in(jax.random.key(seed), part)
    kx, kgap, kstart = jax.random.split(kpart, 3)
    kw = jax.random.split(jax.random.key(seed + 1), 9)
    x = jax.random.normal(kx, (T, D), jnp.float32).astype(jnp.bfloat16)
    gaps = jax.random.randint(kgap, (T,), 1, 4)
    start = jax.random.randint(kstart, (), 0, T)
    seqpos = start + jnp.cumsum(gaps) - gaps[0]
    rows = jnp.arange(T)
    dev = rows // (2 * PIECE)
    off = rows % (2 * PIECE)
    piece = jnp.where(off < PIECE, dev, 2 * NDEV - 1 - dev)
    pos = seqpos[piece * PIECE + off % PIECE].astype(jnp.int32)
    qk = math.sqrt(math.sqrt(math.log(T / 16.0)))

    def nrm(k, shape, scl):
        return (jax.random.normal(k, shape, jnp.float32) * scl).astype(jnp.bfloat16)

    g1 = (1.0 + 0.3 * jax.random.normal(kw[0], (D,), jnp.float32)).astype(jnp.bfloat16)
    g2 = (1.0 + 0.3 * jax.random.normal(kw[1], (D,), jnp.float32)).astype(jnp.bfloat16)
    wq = nrm(kw[2], (D, HQ * DH), qk / math.sqrt(D))
    wk = nrm(kw[3], (D, HKV * DH), qk / math.sqrt(D))
    wv = nrm(kw[4], (D, HKV * DH), 1.0 / math.sqrt(D))
    wo = nrm(kw[5], (HQ * DH, D), 2.0 / math.sqrt(HQ * DH))
    w1 = nrm(kw[6], (D, F), 1.0 / math.sqrt(D))
    w3 = nrm(kw[7], (D, F), 1.0 / math.sqrt(D))
    w2 = nrm(kw[8], (F, D), 1.0 / math.sqrt(F))
    return dict(x=x, pos=pos, g1=g1, g2=g2, wq=wq, wk=wk, wv=wv, wo=wo, w1=w1, w3=w3, w2=w2)


def rms_norm(v, g):
    vf = v.astype(jnp.float32)
    inv = lax.rsqrt(jnp.mean(vf * vf, axis=-1, keepdims=True) + EPS)
    return (vf * inv * g.astype(jnp.float32)).astype(jnp.bfloat16)


def rope(y, p):
    half = DH // 2
    freq = 1.0 / (THETA ** (jnp.arange(0, DH, 2, dtype=jnp.float32) / DH))
    ang = p.astype(jnp.float32)[..., None] * freq
    c = jnp.cos(ang)[..., None, :]
    s = jnp.sin(ang)[..., None, :]
    y1 = y[..., :half]
    y2 = y[..., half:]
    return jnp.concatenate([y1 * c - y2 * s, y2 * c + y1 * s], axis=-1)


def attention(q, k, v, p):
    qr = q.reshape(T // QB, QB, HKV, GRP, DH)
    pr = p.reshape(T // QB, QB)
    kf = k.astype(jnp.float32)
    vf = v.astype(jnp.float32)
    scale = 1.0 / math.sqrt(DH)

    def blk(qp):
        qq, pp = qp
        s = jnp.einsum('qkgd,skd->kgqs', qq.astype(jnp.float32), kf) * scale
        s = jnp.where(p[None, None, None, :] <= pp[None, None, :, None], s, -1e30)
        e = jnp.exp(s - jnp.max(s, axis=-1, keepdims=True))
        w = (e / jnp.sum(e, axis=-1, keepdims=True)).astype(jnp.bfloat16)
        o = jnp.einsum('kgqs,skd->qkgd', w.astype(jnp.float32), vf)
        return o.astype(jnp.bfloat16)

    return lax.map(blk, (qr, pr)).reshape(T, HQ * DH)


def reference(x, pos, g1, g2, wq, wk, wv, wo, w1, w3, w2):
    a = rms_norm(x, g1)
    q = rope(jnp.dot(a, wq, preferred_element_type=jnp.float32).reshape(T, HQ, DH), pos).astype(jnp.bfloat16)
    k = rope(jnp.dot(a, wk, preferred_element_type=jnp.float32).reshape(T, HKV, DH), pos).astype(jnp.bfloat16)
    v = jnp.dot(a, wv, preferred_element_type=jnp.float32).astype(jnp.bfloat16).reshape(T, HKV, DH)
    o = attention(q, k, v, pos)
    h1 = (x.astype(jnp.float32) + jnp.dot(o, wo, preferred_element_type=jnp.float32)).astype(jnp.bfloat16)
    b = rms_norm(h1, g2)
    hid = (jax.nn.silu(jnp.dot(b, w1, preferred_element_type=jnp.float32)) * jnp.dot(b, w3, preferred_element_type=jnp.float32)).astype(jnp.bfloat16)
    return (h1.astype(jnp.float32) + jnp.dot(hid, w2, preferred_element_type=jnp.float32)).astype(jnp.bfloat16)
```

```python
import math
import jax
import jax.numpy as jnp
from jax import lax
from jax.sharding import PartitionSpec as P, NamedSharding

DH = 128
EPS = 1e-5
THETA = 500000.0


def rms_norm(v, g):
    vf = v.astype(jnp.float32)
    inv = lax.rsqrt(jnp.mean(vf * vf, axis=-1, keepdims=True) + EPS)
    return (vf * inv * g.astype(jnp.float32)).astype(jnp.bfloat16)


def rope(y, p):
    half = DH // 2
    freq = 1.0 / (THETA ** (jnp.arange(0, DH, 2, dtype=jnp.float32) / DH))
    ang = p.astype(jnp.float32)[..., None] * freq
    c = jnp.cos(ang)[..., None, :]
    s = jnp.sin(ang)[..., None, :]
    y1 = y[..., :half]
    y2 = y[..., half:]
    return jnp.concatenate([y1 * c - y2 * s, y2 * c + y1 * s], axis=-1)


def attend(q, k, v, qpos, kpos):
    nq, hl, dh = q.shape
    hk = k.shape[1]
    grp = hl // hk
    qb = nq
    while qb % 2 == 0 and qb * hl > 1024:
        qb = qb // 2
    qr = q.reshape(nq // qb, qb, hk, grp, dh)
    pr = qpos.reshape(nq // qb, qb)
    scale = 1.0 / math.sqrt(dh)

    def blk(qp):
        qq, pp = qp
        s = jnp.einsum('qkgd,skd->kgqs', qq, k, preferred_element_type=jnp.float32) * scale
        s = jnp.where(kpos[None, None, None, :] <= pp[None, None, :, None], s, -1e30)
        e = jnp.exp(s - jnp.max(s, axis=-1, keepdims=True))
        w = (e / jnp.sum(e, axis=-1, keepdims=True)).astype(jnp.bfloat16)
        o = jnp.einsum('kgqs,skd->qkgd', w, v, preferred_element_type=jnp.float32)
        return o.astype(jnp.bfloat16)

    return lax.map(blk, (qr, pr)).reshape(nq, hl * dh)


def order(c, nr, ncp):
    i = jnp.arange(nr)
    piece = nr // 4
    dev = 2 * c + i // (2 * piece)
    off = i % (2 * piece)
    return jnp.where(off < piece, dev * piece + off, (4 * ncp - 1 - dev) * piece + off - piece).astype(jnp.int32)


def solution(mesh):
    tok = P(('dp', 'cp', 'tp'), None)
    col = P(None, 'tp')
    row = P('tp', None)

    def local(x, pos, g1, g2, wq, wk, wv, wo, w1, w3, w2):
        a = lax.all_gather(rms_norm(x, g1), 'tp', axis=0, tiled=True)
        pg = lax.all_gather(pos, 'tp', axis=0, tiled=True)
        nr = a.shape[0]
        q = rope(jnp.dot(a, wq, preferred_element_type=jnp.float32).reshape(nr, -1, DH), pg).astype(jnp.bfloat16)
        k = rope(jnp.dot(a, wk, preferred_element_type=jnp.float32).reshape(nr, -1, DH), pg).astype(jnp.bfloat16)
        v = jnp.dot(a, wv, preferred_element_type=jnp.float32).astype(jnp.bfloat16).reshape(nr, -1, DH)
        ka = lax.all_gather(k, 'cp', axis=0, tiled=True)
        va = lax.all_gather(v, 'cp', axis=0, tiled=True)
        ncp = lax.axis_size('cp')
        oq = order(lax.axis_index('cp'), nr, ncp)
        ok = jnp.concatenate([order(c, nr, ncp) for c in range(ncp)])
        o = attend(q, ka, va, oq, ok)
        y = lax.psum_scatter(jnp.dot(o, wo, preferred_element_type=jnp.float32), 'tp', scatter_dimension=0, tiled=True)
        h1 = (x.astype(jnp.float32) + y).astype(jnp.bfloat16)
        b = lax.all_gather(rms_norm(h1, g2), 'tp', axis=0, tiled=True)
        hid = (jax.nn.silu(jnp.dot(b, w1, preferred_element_type=jnp.float32)) * jnp.dot(b, w3, preferred_element_type=jnp.float32)).astype(jnp.bfloat16)
        z = lax.psum_scatter(jnp.dot(hid, w2, preferred_element_type=jnp.float32), 'tp', scatter_dimension=0, tiled=True)
        return (h1.astype(jnp.float32) + z).astype(jnp.bfloat16)

    return jax.shard_map(local, mesh=mesh, in_specs=(tok, P(('dp', 'cp', 'tp')), P(None), P(None), col, col, col, row, col, col, row), out_specs=tok, check_vma=False)
```

```python
import functools
import math

import jax
import jax.numpy as jnp
from jax import lax
from jax.experimental import pallas as pl
from jax.experimental.pallas import tpu as pltpu
from jax.sharding import PartitionSpec as P

DH = 128
EPS = 1e-5
THETA = 500000.0
FC = 512
NS = 8
COLORS = (
    (0, 24, (2, 1, 0)),
    (24, 24, (1, 0, 2)),
    (48, 16, (0, 2, 1)),
)


def layer_kernel(
    x_ref, cs_ref, g1_ref, g2_ref, wq_ref, wk_ref, wv_ref, wo_ref, w1_ref, w3_ref, w2_ref,
    out_ref,
    xa, csa, act, wkv, w1s, w3s, w2s, kv, qb, fm, ob, mb, lb, ot, part, got, gotz, h1, hid,
    wsem, wkvsem, xs, xr, cps, cpr, as_, ar, bs, br, cs_, cr, fs, fr, ys, yr, zs, zr,
):
    j = lax.axis_index('tp')
    c = lax.axis_index('cp')
    co = (c // 16, (c // 4) % 4, c % 4)
    stride = (16, 4, 1)
    dm = x_ref.shape[1]
    nf = w1_ref.shape[1]
    nch = -(-nf // FC)
    pp = x_ref.shape[0] // 2

    def peer(d, t):
        return c + ((co[d] + t) % 4 - co[d]) * stride[d]

    def width(i):
        return min(FC, nf - i * FC)

    def cp_w1(i):
        n = width(i)
        return (pltpu.make_async_copy(w1_ref.at[:, pl.ds(i * FC, n)], w1s.at[i % NS, :, pl.ds(0, n)], wsem.at[0, i % NS]),
                pltpu.make_async_copy(w3_ref.at[:, pl.ds(i * FC, n)], w3s.at[i % NS, :, pl.ds(0, n)], wsem.at[1, i % NS]))

    def cp_w2(i):
        n = width(i)
        s = i % (NS + 1)
        return (pltpu.make_async_copy(w2_ref.at[pl.ds(i * FC, n), :], w2s.at[s, pl.ds(0, n), :], wsem.at[2, s]),)

    def cp_kv():
        return (pltpu.make_async_copy(wk_ref, wkv.at[:, pl.ds(0, DH)], wkvsem.at[0]),
                pltpu.make_async_copy(wv_ref, wkv.at[:, pl.ds(DH, DH)], wkvsem.at[1]))

    def cp_q():
        return (pltpu.make_async_copy(wq_ref.at[:, pl.ds(0, FC)], w1s.at[NS - 1], wsem.at[0, NS - 1]),
                pltpu.make_async_copy(wq_ref.at[:, pl.ds(FC, FC)], w3s.at[NS - 1], wsem.at[1, NS - 1]))

    def cp_o():
        return (pltpu.make_async_copy(wo_ref.at[pl.ds(0, FC), :], w2s.at[NS - 1], wsem.at[2, NS - 1]),
                pltpu.make_async_copy(wo_ref.at[pl.ds(FC, FC), :], w2s.at[NS], wsem.at[2, NS]))

    def start(cps_):
        for q in cps_:
            q.start()

    def wait(cps_):
        for q in cps_:
            q.wait()

    start(cp_kv())
    start(cp_q())

    bar = pltpu.get_barrier_semaphore()
    pl.semaphore_signal(bar, inc=1, device_id={'tp': 1 - j})
    for d in range(3):
        for t in (1, 2, 3):
            pl.semaphore_signal(bar, inc=1, device_id={'cp': peer(d, t)})

    lo = pl.multiple_of(j * pp, pp)
    hi = pl.multiple_of((3 - j) * pp, pp)
    own = (lo, hi)

    for i in range(2):
        xa[pl.ds(own[i], pp), :] = x_ref[pl.ds(i * pp, pp), :]
        csa[pl.ds(own[i], pp), :] = cs_ref[pl.ds(i * pp, pp), :]

    r = lax.broadcasted_iota(jnp.int32, fm.shape[1:], 0)
    qi = lax.broadcasted_iota(jnp.int32, fm.shape[1:], 1) % 32
    rr = r % 32
    cc = ((r // 128 + co[1]) % 4) * 4 + (r // 32 + co[2]) % 4
    fm[0] = cc * 32 + rr - qi
    fm[1] = rr - cc * 32 - qi

    pl.semaphore_wait(bar, 10)

    def cp_x():
        out = []
        for i in range(2):
            out.append(pltpu.make_async_remote_copy(
                x_ref.at[pl.ds(i * pp, pp), :], xa.at[pl.ds(own[i], pp), :], xs.at[i], xr.at[i], device_id={'tp': 1 - j}))
            out.append(pltpu.make_async_remote_copy(
                cs_ref.at[pl.ds(i * pp, pp), :], csa.at[pl.ds(own[i], pp), :], cps.at[i], cpr.at[i], device_id={'tp': 1 - j}))
        return out

    start(cp_x())

    start(cp_o())
    for i in range(min(NS - 1, nch)):
        start(cp_w1(i))
        start(cp_w2(i))

    def norm(v, g):
        vf = v.astype(jnp.float32)
        inv = lax.rsqrt(jnp.mean(vf * vf, axis=-1, keepdims=True) + EPS)
        return (vf * inv * g.astype(jnp.float32)).astype(jnp.bfloat16)

    for q in cp_x():
        q.wait_recv()
    act[...] = norm(xa[...], g1_ref[...])

    ca = csa[:, 0:DH]
    sa = csa[:, DH:2 * DH]

    def rope(u):
        return (u * ca + pltpu.roll(u, DH // 2, 1) * sa).astype(jnp.bfloat16)

    wait(cp_kv())
    kvf = jnp.dot(act[...], wkv[...], preferred_element_type=jnp.float32)
    kv[0, 0, 0, 0] = rope(kvf[:, 0:DH])
    kv[1, 0, 0, 0] = kvf[:, DH:2 * DH].astype(jnp.bfloat16)

    def region(col, sel, half=slice(None)):
        r0, n, order = COLORS[col]
        idx = [0, 0, 0]
        for d, s in zip(order, sel):
            idx[d] = s
        return kv.at[(half, idx[0], idx[1], idx[2], pl.ds(r0, n), slice(None))]

    def cp_a(col, k, t):
        d = COLORS[col][2][k]
        dst = [0, 0, 0]
        dst[k] = (4 - t) % 4
        return pltpu.make_async_remote_copy(
            region(col, (0, 0, 0)), region(col, dst), as_.at[col, k, t - 1], ar.at[col, k, t - 1],
            device_id={'cp': peer(d, t)})

    def cp_b(col, k, t):
        d = COLORS[col][2][k]
        dst = [pl.ds(1, 3), 0, 0]
        dst[k] = (4 - t) % 4
        return pltpu.make_async_remote_copy(
            region(col, (pl.ds(1, 3), 0, 0)), region(col, dst), bs.at[col, k - 1, t - 1], br.at[col, k - 1, t - 1],
            device_id={'cp': peer(d, t)})

    def cp_c(col, t):
        d = COLORS[col][2][2]
        return pltpu.make_async_remote_copy(
            region(col, (pl.ds(0, 4), pl.ds(1, 3), 0)), region(col, (pl.ds(0, 4), pl.ds(1, 3), (4 - t) % 4)),
            cs_.at[col, t // 2], cr.at[col, t // 2], device_id={'cp': peer(d, t)})

    def cp_f(col, t):
        d = COLORS[col][2][2]
        return pltpu.make_async_remote_copy(
            region(col, (pl.ds(0, 4), pl.ds(1, 3), (4 - t) % 4), t // 2),
            region(col, (pl.ds(0, 4), pl.ds(1, 3), 2), t // 2),
            fs.at[col, t // 2], fr.at[col, t // 2], device_id={'cp': peer(d, t)})

    for k in range(3):
        for col in range(3):
            for t in (1, 3, 2):
                cp_a(col, k, t).start()

    wait(cp_q())
    for half, wref in ((0, w1s), (1, w3s)):
        qf = jnp.dot(act[...], wref[NS - 1], preferred_element_type=jnp.float32)
        for h in range(4):
            qh = rope(qf[:, h * DH:(h + 1) * DH])
            hh = half * 4 + h
            qb[0, pl.ds(hh * 32, 32), :] = qh[0:32]
            qb[1, pl.ds(hh * 32, 32), :] = qh[32:64]
    if nch > NS - 1:
        start(cp_w1(NS - 1))

    for col in range(3):
        for t in (1, 3, 2):
            cp_a(col, 0, t).wait_recv()
        for k in (1, 2):
            for t in (1, 3, 2):
                cp_b(col, k, t).start()
    for col in range(3):
        for t in (1, 3, 2):
            cp_a(col, 1, t).wait_recv()
            cp_b(col, 1, t).wait_recv()
        for t in (1, 3):
            cp_c(col, t).start()
    for col in range(3):
        for t in (1, 3):
            cp_c(col, t).wait_recv()
            cp_f(col, t).start()
    for col in range(3):
        for t in (1, 3, 2):
            cp_a(col, 2, t).wait_recv()
            cp_b(col, 2, t).wait_recv()
        for t in (1, 3):
            cp_f(col, t).wait_recv()

    mb[...] = jnp.full_like(mb, -1e30)
    lb[...] = jnp.zeros_like(lb)
    ot[...] = jnp.zeros_like(ot)
    scale = math.log2(math.e) / math.sqrt(DH)
    z = co[0]
    ownp = co[1] * 4 + co[2]

    def unit(u, carry):
        v = u - 4
        first = u < 4
        low = v <= z
        half = jnp.where(first, 1, jnp.where(low, 0, 1))
        reg = jnp.where(first, 0, jnp.where(low, 0, 1))
        blk = jnp.where(first, u, jnp.where(low, v, v - 1))
        lim = jnp.where(first, 1 << 20, jnp.where(low, ownp * 32 + (z - v) * 512, (v - 1 - z) * 512 - ownp * 32))
        dz = (blk - z + 4) % 4
        rows = pl.ds(pl.multiple_of(reg * 32, 32), 32)
        kb = kv[0, dz, :, :, rows, :].reshape(512, DH)
        vb = kv[1, dz, :, :, rows, :].reshape(512, DH)
        s = lax.dot_general(kb, qb[half], (((1,), (1,)), ((), ())), preferred_element_type=jnp.float32) * scale
        s = jnp.where(fm[reg] <= lim, s, -1e30)
        m0 = mb[half]
        m1 = jnp.maximum(m0, jnp.max(s, axis=0, keepdims=True))
        al = jnp.exp2(m0 - m1)
        e = jnp.exp2(s - m1)
        lb[half] = lb[half] * al + jnp.sum(e, axis=0, keepdims=True)
        pv = lax.dot_general(vb, e.astype(jnp.bfloat16), (((0,), (0,)), ((), ())), preferred_element_type=jnp.float32)
        ot[half] = ot[half] * al + pv
        mb[half] = m1
        return carry

    lax.fori_loop(0, 9, unit, 0)

    for half in range(2):
        o = (ot[half] / lb[half]).T.astype(jnp.bfloat16)
        for h in range(8):
            ob[pl.ds(half * 32, 32), pl.ds(h * DH, DH)] = o[h * 32:(h + 1) * 32]

    wait(cp_o())
    part[...] = (jnp.dot(ob[:, 0:FC], w2s[NS - 1], preferred_element_type=jnp.float32)
                 + jnp.dot(ob[:, FC:2 * FC], w2s[NS], preferred_element_type=jnp.float32))
    cp_y = pltpu.make_async_remote_copy(part, got, ys, yr, device_id={'tp': 1 - j})
    cp_y.start()
    for i in (NS - 1, NS):
        if i < nch:
            start(cp_w2(i))
    cp_y.wait()
    h1[...] = (xa[...].astype(jnp.float32) + (part[...] + got[...])).astype(jnp.bfloat16)
    act[...] = norm(h1[...], g2_ref[...])

    def up(i):
        n = width(i)
        wait(cp_w1(i))
        u = jnp.dot(act[...], w1s[i % NS, :, 0:n], preferred_element_type=jnp.float32)
        g = jnp.dot(act[...], w3s[i % NS, :, 0:n], preferred_element_type=jnp.float32)
        hid[i % 2, :, 0:n] = (u * jax.nn.sigmoid(u) * g).astype(jnp.bfloat16)
        if i + NS < nch:
            start(cp_w1(i + NS))

    def down(i):
        n = width(i)
        wait(cp_w2(i))
        zz = jnp.dot(hid[i % 2, :, 0:n], w2s[i % (NS + 1), 0:n, :], preferred_element_type=jnp.float32)
        if i == 0:
            part[...] = zz
        else:
            part[...] += zz
        if i + NS + 1 < nch:
            start(cp_w2(i + NS + 1))

    for i in range(nch + 1):
        if i < nch:
            up(i)
        if i > 0:
            down(i - 1)

    oth = (pl.multiple_of((1 - j) * pp, pp), pl.multiple_of((2 + j) * pp, pp))
    cp_z = [pltpu.make_async_remote_copy(part.at[pl.ds(oth[i], pp), :], gotz.at[pl.ds(i * pp, pp), :], zs.at[i], zr.at[i],
                                         device_id={'tp': 1 - j}) for i in range(2)]
    start(cp_z)
    for i in range(2):
        cp_z[i].wait_recv()
        sl = pl.ds(own[i], pp)
        out_ref[pl.ds(i * pp, pp), :] = (
            h1[sl, :].astype(jnp.float32) + (part[sl, :] + gotz[pl.ds(i * pp, pp), :])).astype(jnp.bfloat16)

    for q in cp_z:
        q.wait_send()
    for q in cp_x():
        q.wait_send()
    for col in range(3):
        for t in (1, 2, 3):
            for k in range(3):
                cp_a(col, k, t).wait_send()
            for k in (1, 2):
                cp_b(col, k, t).wait_send()
        for t in (1, 3):
            cp_c(col, t).wait_send()
            cp_f(col, t).wait_send()


def solution(mesh):
    tok = P(('dp', 'cp', 'tp'), None)
    col = P(None, 'tp')
    row = P('tp', None)

    def local(x, pos, g1, g2, wq, wk, wv, wo, w1, w3, w2):
        rows, dm = x.shape
        freq = 1.0 / (THETA ** (jnp.arange(0, DH, 2, dtype=jnp.float32) / DH))
        ang = pos.astype(jnp.float32)[:, None] * freq
        cos, sin = jnp.cos(ang), jnp.sin(ang)
        cs = jnp.concatenate([cos, cos, -sin, sin], axis=-1)
        bf, f32 = jnp.bfloat16, jnp.float32
        sem = pltpu.SemaphoreType.DMA
        vm = pltpu.VMEM
        vs = pl.BlockSpec(memory_space=pltpu.VMEM)
        anys = pl.BlockSpec(memory_space=pl.ANY)
        scratch = [
            vm((2 * rows, dm), bf),
            vm((2 * rows, 2 * DH), f32),
            vm((2 * rows, dm), bf),
            vm((dm, 2 * DH), bf),
            vm((NS, dm, FC), bf),
            vm((NS, dm, FC), bf),
            vm((NS + 1, FC, dm), bf),
            vm((2, 4, 4, 4, 2 * rows, DH), bf),
            vm((2, 256, DH), bf),
            vm((2, 512, 256), jnp.int32),
            vm((2 * rows, 8 * DH), bf),
            vm((2, 1, 256), f32),
            vm((2, 1, 256), f32),
            vm((2, DH, 256), f32),
            vm((2 * rows, dm), f32),
            vm((2 * rows, dm), f32),
            vm((rows, dm), f32),
            vm((2 * rows, dm), bf),
            vm((2, 2 * rows, FC), bf),
            sem((3, NS + 1)), sem((2,)),
            sem((2,)), sem((2,)), sem((2,)), sem((2,)),
            sem((3, 3, 3)), sem((3, 3, 3)),
            sem((3, 2, 3)), sem((3, 2, 3)),
            sem((3, 2)), sem((3, 2)),
            sem((3, 2)), sem((3, 2)),
            sem, sem, sem((2,)), sem((2,)),
        ]
        return pl.pallas_call(
            layer_kernel,
            name='layer',
            out_shape=jax.ShapeDtypeStruct((rows, dm), bf),
            in_specs=[vs] * 4 + [anys] * 7,
            out_specs=vs,
            scratch_shapes=scratch,
            compiler_params=pltpu.CompilerParams(
                collective_id=0, has_side_effects=True, vmem_limit_bytes=67043328),
        )(x, cs, g1.reshape(1, dm), g2.reshape(1, dm), wq, wk, wv, wo, w1, w3, w2)

    return jax.shard_map(local, mesh=mesh, in_specs=(tok, P(('dp', 'cp', 'tp')), P(None), P(None), col, col, col, row, col, col, row), out_specs=tok, check_vma=False)
```
